32 devices in a mesh: grp: 2 (over y), row: 4 (over z), col: 4 (over x, core).
Axes of the slice: x: 2, y: 2, z: 4, core: 2. Of those that a mesh axis runs over, the one named last changes fastest.
Arguments:
- z_spectra: float32 [32, 2, 2, 4096], P(('grp', 'row', 'col')), parts along dimension 0, may hold values from -6 to 6
- n_spectra: float32 [32, 2, 2, 4096], P(('grp', 'col', 'row')), parts along dimension 0, may hold values from -6 to 6
- z_flags: int32 [32, 2], P(('grp', 'row', 'col')), parts along dimension 0, may hold values 0 or 1
- n_flags: int32 [32, 2], P(('grp', 'col', 'row')), parts along dimension 0, may hold values 0 or 1
- pair_mask: int32 [32, 16], P(('grp', 'row'), 'col'), parts along dimension 0, may hold values 0 or 1
Outputs:
- stacks: float32 [32, 16, 512], P(('grp', 'row'), 'col'), parts along dimension 0
The draws below stay inside these ranges and needn't reach their ends.
There are 2 independent parts, one for each index of `grp`. The reference program is written for one: setup_inputs(seed, part) draws one part's arguments, and reference() takes and returns one part's arrays. A program takes and returns all parts, laid end to end along the dimension named above; each array names one. Nothing has to cross between parts.
All inputs are finite; a program needn't handle non-finite values. No bound on the sum of `z_flags` or of `n_flags` or of `pair_mask` on one device may be relied on, other than what follows from the above.
Results may differ from the reference program's by a relative error of at most 0.0037.
Values sent between devices are 32-bit elements; how exact they have to be, the bound alone decides.
A program may use at most 64 MiB of HBM per device.

```python
import math
import jax
import jax.numpy as jnp
from jax import lax

F = 4096
LAGS = 512
WIN = 2
S = 16


def place_ends(drawn, own_key, smallest, high):
    longest = drawn.shape.index(max(drawn.shape))
    spots = []
    for shift in (0, 1):
        where = [jax.random.randint(jax.random.fold_in(own_key, axis), (), 0, length) for axis, length in enumerate(drawn.shape)]
        where[longest] = (where[longest] + shift) % drawn.shape[longest]
        spots.append(tuple(where))
    return drawn.at[spots[0]].set(smallest).at[spots[1]].set(high)


def block_levels(stream_key, shape, pieces, least, high):
    def one(dim, blocks):
        steps = jax.random.uniform(jax.random.fold_in(jax.random.fold_in(stream_key, 6), dim), (blocks,), jnp.float32, least / len(pieces), high / len(pieces))
        return jnp.repeat(jnp.exp(steps), shape[dim] // blocks).reshape((-1,) + (1,) * (len(shape) - dim - 1))

    gain = one(*pieces[0])
    for cut in pieces[1:]:
        gain = gain * one(*cut)
    return gain


def scatter_about(stream_key, dims, scale, most, pieces=(), kind=jnp.bfloat16):
    loudness = block_levels(stream_key, dims, pieces, -0.22, 0.18) if pieces else 1.0
    array = jax.random.normal(stream_key, dims, jnp.float32) * scale * loudness
    return jnp.minimum(jnp.maximum(array, -most), most).astype(kind)


def setup_inputs(seed: int = 0, part: int = 0) -> dict:
    streams_of = jax.random.split(jax.random.key(seed), 6)
    part_splits = jax.random.split(jax.random.fold_in(streams_of[5], part), 6)
    z_spectra = scatter_about(part_splits[0], (S, WIN, 2, F), 1.0, 6.0, ((0, 16),), jnp.float32)
    n_spectra = scatter_about(part_splits[1], (S, WIN, 2, F), 1.0, 6.0, ((0, 16),), jnp.float32)
    z_flags = place_ends((jax.random.randint(part_splits[2], (S, WIN), 0, 5) < 4).astype(jnp.int32), jax.random.fold_in(part_splits[2], 1), 0, 1)
    n_flags = place_ends((jax.random.randint(part_splits[3], (S, WIN), 0, 5) < 4).astype(jnp.int32), jax.random.fold_in(part_splits[3], 1), 0, 1)
    pair_mask = place_ends((jax.random.randint(part_splits[4], (S, S), 0, 4) < 3).astype(jnp.int32), jax.random.fold_in(part_splits[4], 1), 0, 1)
    return {"z_spectra": z_spectra, "n_spectra": n_spectra, "z_flags": z_flags, "n_flags": n_flags, "pair_mask": pair_mask}


def lag_table(first_bin, bin_count, total_bins, lag_count):
    freq_bins = first_bin + jnp.arange(bin_count, dtype=jnp.int32)
    lag_steps = jnp.arange(lag_count, dtype=jnp.int32) - lag_count // 2
    phase_index = freq_bins[:, None] * lag_steps[None, :] % (2 * total_bins)
    angles = phase_index.astype(jnp.float32) * (math.pi / total_bins)
    weight = jnp.where(freq_bins == 0, 1.0, 2.0).astype(jnp.float32)[:, None]
    return jnp.concatenate([weight * jnp.cos(angles), -weight * jnp.sin(angles)], 0).astype(jnp.bfloat16)

def correlate(row_spec, col_spec, lag_tab):
    z_real = row_spec[:, None, :, 0, :]
    z_imag = row_spec[:, None, :, 1, :]
    n_real = col_spec[None, :, :, 0, :]
    n_imag = col_spec[None, :, :, 1, :]
    real_part = z_real * n_real + z_imag * n_imag
    imag_part = z_imag * n_real - z_real * n_imag
    row_count, col_count, windows, bins = real_part.shape
    cross_spec = jnp.stack([real_part, imag_part], 3).astype(jnp.bfloat16)
    merged = cross_spec.reshape(row_count * col_count * windows, 2 * bins)
    product = jnp.dot(merged, lag_tab, preferred_element_type=jnp.float32)
    return product.reshape(row_count, col_count, windows, lag_tab.shape[1])

def stack_windows(corr, pair_marks):
    spread = jnp.sqrt(lax.optimization_barrier(jnp.mean(corr * corr, -1, keepdims=True)) + 1e-05)
    unit_corr = corr / spread
    window_count = jnp.maximum(lax.optimization_barrier(jnp.sum(pair_marks, -1)), 1.0)
    summed = lax.optimization_barrier(jnp.sum(pair_marks[..., None] * unit_corr, -2))
    return summed / window_count[..., None]

def reference(z_spectra, n_spectra, z_flags, n_flags, pair_mask):
    lag_tab = lag_table(0, F, F, LAGS)
    z_marks = z_flags.astype(jnp.float32)
    n_marks = n_flags.astype(jnp.float32)

    def one_station(inputs):
        z_row, z_mark = inputs
        corr = correlate(z_row[None], n_spectra, lag_tab)[0]
        return stack_windows(corr, z_mark[None, :] * n_marks)
    stacked = lax.map(one_station, (z_spectra, z_marks))
    return stacked * pair_mask.astype(jnp.float32)[..., None]
```

```python
import functools
import math

import jax
import jax.numpy as jnp
import numpy as np
from jax import lax
from jax.experimental import pallas as pl
from jax.experimental.pallas import tpu as pltpu
from jax.sharding import PartitionSpec as P

LAGS = 512
LANES = 128
MESH = pl.DeviceIdType.MESH


def tables(bins):
    rows, blocks = bins // LANES, LAGS // LANES
    period = 2 * rows
    kt, short = np.arange(rows), np.arange(period)
    phi = 2 * np.pi * ((short[:, None] * kt[None, :]) % period) / period
    inner = np.block([[np.cos(phi), -np.sin(phi)], [np.sin(phi), np.cos(phi)]])
    lane, t0 = np.arange(LANES), np.arange(LANES)
    psi = np.pi * (t0[:, None] * lane[None, :]) / bins
    turn = np.stack([np.cos(psi), np.sin(psi)]).astype(np.float32)
    hop = np.arange(blocks) - blocks // 2
    chi = np.pi * ((LANES * hop[:, None] * lane[None, :]) % (2 * bins)) / bins
    outer = np.concatenate([np.cos(chi), -np.sin(chi)], 1).astype(np.float32)
    high = outer.astype(jnp.bfloat16)
    low = (outer - high.astype(np.float32)).astype(jnp.bfloat16)
    return inner.astype(jnp.bfloat16), turn, np.concatenate([high, low], 0)


def kernel(R, C, z_hbm, n_hbm, zf_hbm, nf_hbm, mask_hbm, inner_hbm, turn_hbm, outer_hbm, out_ref,
           z_buf, n_buf, zf_buf, nf_buf, mask_buf, inner, turn, outer,
           load_sem, z_send, z_recv, zf_send, zf_recv, right_send, left_send, n_recv,
           rf_send, lf_send, nf_recv):
    row, col = lax.axis_index("row"), lax.axis_index("col")
    W = z_buf.shape[1]
    bin_rows = z_buf.shape[2] // 2
    period = inner.shape[0] // 2
    blocks = outer.shape[0] // 2

    loads = [
        pltpu.make_async_copy(n_hbm.at[0], n_buf.at[row], load_sem.at[0]),
        pltpu.make_async_copy(z_hbm.at[0], z_buf.at[col], load_sem.at[1]),
        pltpu.make_async_copy(nf_hbm, nf_buf.at[row], load_sem.at[2]),
        pltpu.make_async_copy(zf_hbm, zf_buf.at[col], load_sem.at[3]),
        pltpu.make_async_copy(mask_hbm, mask_buf, load_sem.at[4]),
        pltpu.make_async_copy(inner_hbm, inner, load_sem.at[5]),
        pltpu.make_async_copy(turn_hbm, turn, load_sem.at[6]),
        pltpu.make_async_copy(outer_hbm, outer, load_sem.at[7]),
    ]
    for load in loads:
        load.start()

    has_left, has_right = row > 0, row < R - 1

    barrier = pltpu.get_barrier_semaphore()

    @pl.when(has_left)
    def _():
        pl.semaphore_signal(barrier, inc=1, device_id={"row": row - 1}, device_id_type=MESH)

    @pl.when(has_right)
    def _():
        pl.semaphore_signal(barrier, inc=1, device_id={"row": row + 1}, device_id_type=MESH)

    for step in range(1, C):
        pl.semaphore_signal(barrier, inc=1, device_id={"col": lax.rem(col + step, C)}, device_id_type=MESH)
    greeted = C - 1 + jnp.where(has_left, 1, 0) + jnp.where(has_right, 1, 0)
    pl.semaphore_wait(barrier, greeted)

    def spectrum(owner, w, send, to):
        return pltpu.make_async_remote_copy(
            n_buf.at[owner, w], n_buf.at[owner, w], send.at[owner, w], n_recv.at[owner, w],
            device_id={"row": to}, device_id_type=MESH)

    def flag(owner, send, to):
        return pltpu.make_async_remote_copy(
            nf_buf.at[owner], nf_buf.at[owner], send.at[owner], nf_recv.at[owner],
            device_id={"row": to}, device_id_type=MESH)

    def z_copy(owner, w, to):
        return pltpu.make_async_remote_copy(
            z_buf.at[owner, w], z_buf.at[owner, w], z_send.at[to, w], z_recv.at[owner, w],
            device_id={"col": to}, device_id_type=MESH)

    def zf_copy(owner, to):
        return pltpu.make_async_remote_copy(
            zf_buf.at[owner], zf_buf.at[owner], zf_send.at[to], zf_recv.at[owner],
            device_id={"col": to}, device_id_type=MESH)

    loads[2].wait()
    loads[0].wait()

    @pl.when(has_right)
    def _():
        flag(row, rf_send, row + 1).start()
        for w in range(W):
            spectrum(row, w, right_send, row + 1).start()

    @pl.when(has_left)
    def _():
        flag(row, lf_send, row - 1).start()
        for w in range(W):
            spectrum(row, w, left_send, row - 1).start()

    loads[3].wait()
    loads[1].wait()
    for step in range(1, C):
        zf_copy(col, lax.rem(col + step, C)).start()
    for w in range(W):
        for step in range(1, C):
            z_copy(col, w, lax.rem(col + step, C)).start()
    for load in loads[4:]:
        load.wait()

    spot = lax.broadcasted_iota(jnp.int32, (bin_rows, LANES), 0) + lax.broadcasted_iota(
        jnp.int32, (bin_rows, LANES), 1)
    weight = jnp.where(spot == 0, 1.0, 2.0).astype(jnp.float32)

    def unit(owner, w):
        n_real = n_buf[owner, w, pl.ds(0, bin_rows, stride=2), :] * weight
        n_imag = n_buf[owner, w, pl.ds(1, bin_rows, stride=2), :] * weight
        cross = []
        for i in range(C):
            z_real = z_buf[i, w, pl.ds(0, bin_rows, stride=2), :]
            z_imag = z_buf[i, w, pl.ds(1, bin_rows, stride=2), :]
            cross.append(jnp.concatenate(
                [z_real * n_real + z_imag * n_imag, z_imag * n_real - z_real * n_imag], 0
            ).astype(jnp.bfloat16))
        short = jnp.dot(inner[...], jnp.concatenate(cross, 1), preferred_element_type=jnp.float32)
        turned = []
        for i in range(C):
            real = short[:period, i * LANES:(i + 1) * LANES]
            imag = short[period:, i * LANES:(i + 1) * LANES]
            for part in range(LANES // period):
                cosine = turn[0, part * period:(part + 1) * period, :]
                sine = turn[1, part * period:(part + 1) * period, :]
                turned.append(jnp.concatenate(
                    [real * cosine - imag * sine, real * sine + imag * cosine], 1).astype(jnp.bfloat16))
        lags = lax.dot_general(outer[...], jnp.concatenate(turned, 0), (((1,), (1,)), ((), ())),
                               preferred_element_type=jnp.float32)
        lags = lags[:blocks] + lags[blocks:]
        n_flag = nf_buf[owner].astype(jnp.float32)
        mask = mask_buf[...].astype(jnp.float32)
        here = lax.broadcasted_iota(jnp.int32, mask.shape, 1) == owner
        kept = jnp.sum(jnp.where(here, mask, 0.0), axis=1, keepdims=True)
        for i in range(C):
            corr = lags[:, i * LANES:(i + 1) * LANES]
            marks = zf_buf[i].astype(jnp.float32) * n_flag
            count = jnp.maximum(jnp.sum(marks, axis=1, keepdims=True), 1.0)
            power = jnp.sum(jnp.sum(corr * corr, axis=0, keepdims=True), axis=1, keepdims=True)
            spread = jnp.sqrt(power / LAGS + 1e-05)
            gain = marks[:, w:w + 1] * kept[i:i + 1] / (count * spread)
            place = pl.ds(i * blocks * R + owner, blocks, stride=R)
            if w == 0:
                out_ref[place, :] = corr * gain
            else:
                out_ref[place, :] += corr * gain

    def arrive(owner, w, forward, send, f_send, to):
        if w == 0:
            flag(owner, f_send, to).wait_recv()
        spectrum(owner, w, send, to).wait_recv()

        @pl.when(forward)
        def _():
            if w == 0:
                flag(owner, f_send, to).start()
            spectrum(owner, w, send, to).start()

    def collect(step):
        for w in range(W):
            @pl.when(row - step >= 0)
            def _():
                arrive(row - step, w, has_right, right_send, rf_send, lax.rem(row + 1, R))

            @pl.when(row + step < R)
            def _():
                arrive(row + step, w, has_left, left_send, lf_send, lax.rem(row + R - 1, R))

    def compute(step):
        @pl.when(row - step >= 0)
        def _():
            for w in range(W):
                unit(row - step, w)

        @pl.when(row + step < R)
        def _():
            for w in range(W):
                unit(row + step, w)

    collect(1)
    for step in range(1, C):
        zf_copy(lax.rem(col + C - step, C), lax.rem(col + step, C)).wait_recv()
    for w in range(W):
        for step in range(1, C):
            z_copy(lax.rem(col + C - step, C), w, lax.rem(col + step, C)).wait_recv()
        unit(row, w)

    @pl.loop(2, R)
    def _(step):
        collect(step)
        compute(step - 1)

    compute(R - 1)

    for step in range(1, C):
        zf_copy(col, lax.rem(col + step, C)).wait_send()
        for w in range(W):
            z_copy(col, w, lax.rem(col + step, C)).wait_send()

    @pl.loop(0, R)
    def _(owner):
        @pl.when(has_right & (owner <= row))
        def _():
            flag(owner, rf_send, lax.rem(row + 1, R)).wait_send()
            for w in range(W):
                spectrum(owner, w, right_send, lax.rem(row + 1, R)).wait_send()

        @pl.when(has_left & (owner >= row))
        def _():
            flag(owner, lf_send, lax.rem(row + R - 1, R)).wait_send()
            for w in range(W):
                spectrum(owner, w, left_send, lax.rem(row + R - 1, R)).wait_send()


def body(R, C, z_spectra, n_spectra, z_flags, n_flags, pair_mask):
    windows, bins = z_spectra.shape[1], z_spectra.shape[3]
    rows, blocks = bins // LANES, LAGS // LANES
    inner, turn, outer = tables(bins)

    def interleave(x):
        return x.reshape(1, windows, 2, rows, LANES).transpose(0, 1, 3, 2, 4).reshape(
            1, windows, 2 * rows, LANES)

    DMA = pltpu.SemaphoreType.DMA
    out = pl.pallas_call(
        functools.partial(kernel, R, C),
        out_shape=jax.ShapeDtypeStruct((C * blocks * R, LANES), jnp.float32),
        in_specs=[pl.BlockSpec(memory_space=pl.ANY)] * 8,
        out_specs=pl.BlockSpec(memory_space=pltpu.VMEM),
        scratch_shapes=[
            pltpu.VMEM((C, windows, 2 * rows, LANES), jnp.float32),
            pltpu.VMEM((R, windows, 2 * rows, LANES), jnp.float32),
            pltpu.VMEM((C, 1, windows), jnp.int32),
            pltpu.VMEM((R, 1, windows), jnp.int32),
            pltpu.VMEM(pair_mask.shape, jnp.int32),
            pltpu.VMEM(inner.shape, jnp.bfloat16),
            pltpu.VMEM(turn.shape, jnp.float32),
            pltpu.VMEM(outer.shape, jnp.bfloat16),
            DMA((8,)),
            DMA((C, windows)), DMA((C, windows)), DMA((C,)), DMA((C,)),
            DMA((R, windows)), DMA((R, windows)), DMA((R, windows)),
            DMA((R,)), DMA((R,)), DMA((R,)),
        ],
        compiler_params=pltpu.CompilerParams(collective_id=0, has_side_effects=True),
        name="correlate",
    )(interleave(z_spectra), interleave(n_spectra), z_flags, n_flags, pair_mask,
      jnp.asarray(inner), jnp.asarray(turn), jnp.asarray(outer))
    return out.reshape(C, blocks, R, LANES).transpose(0, 2, 1, 3).reshape(C, R, LAGS)


def solution(mesh):
    placed = (
        P(("grp", "row", "col"), None, None, None),
        P(("grp", "col", "row"), None, None, None),
        P(("grp", "row", "col"), None),
        P(("grp", "col", "row"), None),
        P(("grp", "row"), "col"),
    )
    return jax.shard_map(
        functools.partial(body, mesh.shape["row"], mesh.shape["col"]), mesh=mesh,
        in_specs=placed, out_specs=P(("grp", "row"), "col", None), check_vma=False,
    )
```

```python
import functools
import math

import jax
import jax.numpy as jnp
import numpy as np
from jax import lax
from jax.experimental import pallas as pl
from jax.experimental.pallas import tpu as pltpu
from jax.sharding import PartitionSpec as P

LAGS = 512
LANES = 128
MESH = pl.DeviceIdType.MESH
REACH = 3


def tables(bins):
    rows, blocks = bins // LANES, LAGS // LANES
    period = 2 * rows
    kt, short = np.arange(rows), np.arange(period)
    phi = 2 * np.pi * ((short[:, None] * kt[None, :]) % period) / period
    inner = np.block([[np.cos(phi), -np.sin(phi)], [np.sin(phi), np.cos(phi)]])
    lane, t0 = np.arange(LANES), np.arange(LANES)
    psi = np.pi * (t0[:, None] * lane[None, :]) / bins
    turn = np.stack([np.cos(psi), np.sin(psi)]).astype(np.float32)
    hop = np.arange(blocks) - blocks // 2
    chi = np.pi * ((LANES * hop[:, None] * lane[None, :]) % (2 * bins)) / bins
    outer = np.concatenate([np.cos(chi), -np.sin(chi)], 1).astype(np.float32)
    high = outer.astype(jnp.bfloat16)
    low = (outer - high.astype(np.float32)).astype(jnp.bfloat16)
    return inner.astype(jnp.bfloat16), turn, np.concatenate([high, low], 0)


def kernel(R, C, reach, z_hbm, n_hbm, zf_hbm, nf_hbm, mask_hbm, inner_hbm, turn_hbm, outer_hbm, out_ref,
           z_buf, n_buf, zf_buf, nf_buf, mask_buf, inner, turn, outer,
           load_sem, z_send, z_recv, zf_send, zf_recv, right_send, left_send, n_recv,
           rf_send, lf_send, nf_recv, own_send, own_f_send, ready):
    row, col = lax.axis_index("row"), lax.axis_index("col")
    W = z_buf.shape[1]
    bin_rows = z_buf.shape[2] // 2
    period = inner.shape[0] // 2
    blocks = outer.shape[0] // 2

    loads = [
        pltpu.make_async_copy(n_hbm.at[0], n_buf.at[row], load_sem.at[0]),
        pltpu.make_async_copy(z_hbm.at[0], z_buf.at[col], load_sem.at[1]),
        pltpu.make_async_copy(nf_hbm, nf_buf.at[row], load_sem.at[2]),
        pltpu.make_async_copy(zf_hbm, zf_buf.at[col], load_sem.at[3]),
        pltpu.make_async_copy(mask_hbm, mask_buf, load_sem.at[4]),
        pltpu.make_async_copy(inner_hbm, inner, load_sem.at[5]),
        pltpu.make_async_copy(turn_hbm, turn, load_sem.at[6]),
        pltpu.make_async_copy(outer_hbm, outer, load_sem.at[7]),
    ]
    for load in loads:
        load.start()

    has_left, has_right = row > 0, row < R - 1
    barrier = pltpu.get_barrier_semaphore()

    def there(hop):
        return (row + hop < R) if hop > 0 else (row + hop >= 0)

    for hop in (-1, 1):
        @pl.when(there(hop))
        def _():
            pl.semaphore_signal(barrier, inc=1, device_id={"row": row + hop}, device_id_type=MESH)

    for step in range(1, C):
        pl.semaphore_signal(barrier, inc=1, device_id={"col": lax.rem(col + step, C)}, device_id_type=MESH)
    pl.semaphore_wait(barrier, C - 1 + jnp.where(has_left, 1, 0) + jnp.where(has_right, 1, 0))

    def tell(hop):
        far = abs(hop) + 1
        back = -1 if hop > 0 else 1
        if far <= reach:
            @pl.when(there(hop) & there(back))
            def _():
                pl.semaphore_signal(ready.at[int(hop < 0), far], inc=1,
                                    device_id={"row": row + back}, device_id_type=MESH)

    def learn(hop):
        @pl.when(there(hop))
        def _():
            pl.semaphore_wait(ready.at[int(hop < 0), abs(hop)], 1)

    tell(1)
    tell(-1)

    def spectrum(owner, w, send, to):
        return pltpu.make_async_remote_copy(
            n_buf.at[owner, w], n_buf.at[owner, w], send.at[owner, w], n_recv.at[owner, w],
            device_id={"row": to}, device_id_type=MESH)

    def flag(owner, send, to):
        return pltpu.make_async_remote_copy(
            nf_buf.at[owner], nf_buf.at[owner], send.at[owner], nf_recv.at[owner],
            device_id={"row": to}, device_id_type=MESH)

    def z_copy(owner, w, to):
        return pltpu.make_async_remote_copy(
            z_buf.at[owner, w], z_buf.at[owner, w], z_send.at[to, w], z_recv.at[owner, w],
            device_id={"col": to}, device_id_type=MESH)

    def zf_copy(owner, to):
        return pltpu.make_async_remote_copy(
            zf_buf.at[owner], zf_buf.at[owner], zf_send.at[to], zf_recv.at[owner],
            device_id={"col": to}, device_id_type=MESH)

    def own_copy(hop, w):
        side, far = int(hop < 0), abs(hop) - 1
        return pltpu.make_async_remote_copy(
            n_buf.at[row, w], n_buf.at[row, w], own_send.at[side, far, w], n_recv.at[row, w],
            device_id={"row": row + hop}, device_id_type=MESH)

    def own_flag(hop):
        side, far = int(hop < 0), abs(hop) - 1
        return pltpu.make_async_remote_copy(
            nf_buf.at[row], nf_buf.at[row], own_f_send.at[side, far], nf_recv.at[row],
            device_id={"row": row + hop}, device_id_type=MESH)

    def send_own(hop):
        @pl.when(there(hop))
        def _():
            own_flag(hop).start()
            for w in range(W):
                own_copy(hop, w).start()

    for hop in range(2, reach + 1):
        learn(-hop)
        tell(-hop)
    loads[2].wait()
    loads[0].wait()
    for hop in range(reach, 0, -1):
        send_own(-hop)
    send_own(1)
    loads[3].wait()
    loads[1].wait()
    for step in range(1, C):
        zf_copy(col, lax.rem(col + step, C)).start()
    for w in range(W):
        for step in range(1, C):
            z_copy(col, w, lax.rem(col + step, C)).start()
    for hop in range(2, reach + 1):
        learn(hop)
        tell(hop)
        send_own(hop)
    for load in loads[4:]:
        load.wait()

    spot = lax.broadcasted_iota(jnp.int32, (bin_rows, LANES), 0) + lax.broadcasted_iota(
        jnp.int32, (bin_rows, LANES), 1)
    weight = jnp.where(spot == 0, 1.0, 2.0).astype(jnp.float32)

    def unit(owner):
        pairs = [(i, w) for i in range(C) for w in range(W)]
        n_real = [n_buf[owner, w, pl.ds(0, bin_rows, stride=2), :] * weight for w in range(W)]
        n_imag = [n_buf[owner, w, pl.ds(1, bin_rows, stride=2), :] * weight for w in range(W)]
        cross = []
        for i, w in pairs:
            z_real = z_buf[i, w, pl.ds(0, bin_rows, stride=2), :]
            z_imag = z_buf[i, w, pl.ds(1, bin_rows, stride=2), :]
            cross.append(jnp.concatenate(
                [z_real * n_real[w] + z_imag * n_imag[w], z_imag * n_real[w] - z_real * n_imag[w]], 0
            ).astype(jnp.bfloat16))
        short = jnp.dot(inner[...], jnp.concatenate(cross, 1), preferred_element_type=jnp.float32)
        turned = []
        for at in range(len(pairs)):
            real = short[:period, at * LANES:(at + 1) * LANES]
            imag = short[period:, at * LANES:(at + 1) * LANES]
            for part in range(LANES // period):
                cosine = turn[0, part * period:(part + 1) * period, :]
                sine = turn[1, part * period:(part + 1) * period, :]
                turned.append(jnp.concatenate(
                    [real * cosine - imag * sine, real * sine + imag * cosine], 1).astype(jnp.bfloat16))
        lags = lax.dot_general(outer[...], jnp.concatenate(turned, 0), (((1,), (1,)), ((), ())),
                               preferred_element_type=jnp.float32)
        lags = lags[:blocks] + lags[blocks:]
        n_flag = nf_buf[owner].astype(jnp.float32)
        mask = mask_buf[...].astype(jnp.float32)
        here = lax.broadcasted_iota(jnp.int32, mask.shape, 1) == owner
        kept = jnp.sum(jnp.where(here, mask, 0.0), axis=1, keepdims=True)
        for i in range(C):
            marks = zf_buf[i].astype(jnp.float32) * n_flag
            count = jnp.maximum(jnp.sum(marks, axis=1, keepdims=True), 1.0)
            gain = marks * kept[i:i + 1] / count
            total = jnp.zeros((blocks, LANES), jnp.float32)
            for w in range(W):
                at = i * W + w
                corr = lags[:, at * LANES:(at + 1) * LANES]
                power = jnp.sum(jnp.sum(corr * corr, axis=0, keepdims=True), axis=1, keepdims=True)
                spread = jnp.sqrt(power / LAGS + 1e-05)
                total = total + corr * (gain[:, w:w + 1] / spread)
            out_ref[pl.ds(i * blocks * R + owner, blocks, stride=R), :] = total

    def arrive(owner, w, forward, send, f_send, to):
        if w == 0:
            flag(owner, f_send, to).wait_recv()
        spectrum(owner, w, send, to).wait_recv()
        if forward is False:
            return

        @pl.when(forward)
        def _():
            if w == 0:
                flag(owner, f_send, to).start()
            spectrum(owner, w, send, to).start()

    for step in range(1, C):
        zf_copy(lax.rem(col + C - step, C), lax.rem(col + step, C)).wait_recv()
    for w in range(W):
        for step in range(1, C):
            z_copy(lax.rem(col + C - step, C), w, lax.rem(col + step, C)).wait_recv()
    unit(row)

    def take(p):
        left = p <= row
        owner = jnp.where(left, row - p, p)
        if reach == R - 1:
            for w in range(W):
                arrive(owner, w, False, right_send, rf_send, lax.rem(row + 1, R))
        else:
            @pl.when(left)
            def _():
                for w in range(W):
                    arrive(owner, w, has_right & (p >= reach), right_send, rf_send, lax.rem(row + 1, R))

            @pl.when(p > row)
            def _():
                for w in range(W):
                    arrive(owner, w, has_left & (p - row >= reach), left_send, lf_send,
                           lax.rem(row + R - 1, R))
        unit(owner)

    if R <= 4:
        for p in range(1, R):
            take(p)
    else:
        pl.loop(1, R)(take)

    hops = [sign * hop for hop in range(1, reach + 1) for sign in (1, -1)]
    for hop in hops:
        @pl.when(there(hop))
        def _():
            own_flag(hop).wait_send()
            for w in range(W):
                own_copy(hop, w).wait_send()

    for step in range(1, C):
        zf_copy(col, lax.rem(col + step, C)).wait_send()
        for w in range(W):
            z_copy(col, w, lax.rem(col + step, C)).wait_send()

    if reach == R - 1:
        return

    @pl.loop(0, R)
    def _(owner):
        @pl.when(has_right & (owner <= row - reach))
        def _():
            flag(owner, rf_send, lax.rem(row + 1, R)).wait_send()
            for w in range(W):
                spectrum(owner, w, right_send, lax.rem(row + 1, R)).wait_send()

        @pl.when(has_left & (owner >= row + reach))
        def _():
            flag(owner, lf_send, lax.rem(row + R - 1, R)).wait_send()
            for w in range(W):
                spectrum(owner, w, left_send, lax.rem(row + R - 1, R)).wait_send()


def body(R, C, z_spectra, n_spectra, z_flags, n_flags, pair_mask):
    windows, bins = z_spectra.shape[1], z_spectra.shape[3]
    rows, blocks = bins // LANES, LAGS // LANES
    inner, turn, outer = tables(bins)

    def interleave(x):
        return x.reshape(1, windows, 2, rows, LANES).transpose(0, 1, 3, 2, 4).reshape(
            1, windows, 2 * rows, LANES)

    reach = min(REACH, R - 1)
    DMA = pltpu.SemaphoreType.DMA
    out = pl.pallas_call(
        functools.partial(kernel, R, C, reach),
        out_shape=pltpu.VMEM((C * blocks * R, LANES), jnp.float32),
        in_specs=[pl.BlockSpec(memory_space=pl.ANY)] * 8,
        out_specs=pl.BlockSpec(memory_space=pltpu.VMEM),
        scratch_shapes=[
            pltpu.VMEM((C, windows, 2 * rows, LANES), jnp.float32),
            pltpu.VMEM((R, windows, 2 * rows, LANES), jnp.float32),
            pltpu.VMEM((C, 1, windows), jnp.int32),
            pltpu.VMEM((R, 1, windows), jnp.int32),
            pltpu.VMEM(pair_mask.shape, jnp.int32),
            pltpu.VMEM(inner.shape, jnp.bfloat16),
            pltpu.VMEM(turn.shape, jnp.float32),
            pltpu.VMEM(outer.shape, jnp.bfloat16),
            DMA((8,)),
            DMA((C, windows)), DMA((C, windows)), DMA((C,)), DMA((C,)),
            DMA((R, windows)), DMA((R, windows)), DMA((R, windows)),
            DMA((R,)), DMA((R,)), DMA((R,)),
            DMA((2, reach, windows)), DMA((2, reach)), pltpu.SemaphoreType.REGULAR((2, reach + 1)),
        ],
        compiler_params=pltpu.CompilerParams(collective_id=0, has_side_effects=True),
        name="correlate",
    )(interleave(z_spectra), interleave(n_spectra), z_flags, n_flags, pair_mask,
      jnp.asarray(inner), jnp.asarray(turn), jnp.asarray(outer))
    return out.reshape(C, blocks, R, LANES).transpose(0, 2, 1, 3).reshape(C, R, LAGS)


def solution(mesh):
    placed = (
        P(("grp", "row", "col"), None, None, None),
        P(("grp", "col", "row"), None, None, None),
        P(("grp", "row", "col"), None),
        P(("grp", "col", "row"), None),
        P(("grp", "row"), "col"),
    )
    return jax.shard_map(
        functools.partial(body, mesh.shape["row"], mesh.shape["col"]), mesh=mesh,
        in_specs=placed, out_specs=P(("grp", "row"), "col", None), check_vma=False,
    )
```

```python
import functools
import math

import jax
import jax.numpy as jnp
import numpy as np
from jax import lax
from jax.experimental import pallas as pl
from jax.experimental.pallas import tpu as pltpu
from jax.sharding import PartitionSpec as P

LAGS = 512
LANES = 128
MESH = pl.DeviceIdType.MESH
REACH = 3


def tables(bins):
    rows, blocks = bins // LANES, LAGS // LANES
    period = 2 * rows
    kt, short = np.arange(rows), np.arange(period)
    phi = 2 * np.pi * ((short[:, None] * kt[None, :]) % period) / period
    inner = np.block([[np.cos(phi), -np.sin(phi)], [np.sin(phi), np.cos(phi)]])
    lane, t0 = np.arange(LANES), np.arange(LANES)
    psi = np.pi * (t0[:, None] * lane[None, :]) / bins
    turn = np.stack([np.cos(psi), np.sin(psi)]).astype(np.float32)
    hop = np.arange(blocks) - blocks // 2
    chi = np.pi * ((LANES * hop[:, None] * lane[None, :]) % (2 * bins)) / bins
    outer = np.concatenate([np.cos(chi), -np.sin(chi)], 1).astype(np.float32)
    high = outer.astype(jnp.bfloat16)
    low = (outer - high.astype(np.float32)).astype(jnp.bfloat16)
    return inner.astype(jnp.bfloat16), turn, np.concatenate([high, low], 0)


def kernel(R, C, reach, z_hbm, n_hbm, zf_hbm, nf_hbm, mask_hbm, inner_hbm, turn_hbm, outer_hbm, out_ref,
           z_buf, n_buf, zf_buf, nf_buf, mask_buf, inner, turn, outer,
           load_sem, z_send, z_recv, zf_send, zf_recv, right_send, left_send, n_recv,
           rf_send, lf_send, nf_recv, own_send, own_f_send, ready, turn_sem):
    row, col = lax.axis_index("row"), lax.axis_index("col")
    W = z_buf.shape[1]
    bin_rows = z_buf.shape[2] // 2
    period = inner.shape[0] // 2
    blocks = outer.shape[0] // 2

    loads = [
        pltpu.make_async_copy(n_hbm.at[0], n_buf.at[row], load_sem.at[0]),
        pltpu.make_async_copy(z_hbm.at[0], z_buf.at[col], load_sem.at[1]),
        pltpu.make_async_copy(nf_hbm, nf_buf.at[row], load_sem.at[2]),
        pltpu.make_async_copy(zf_hbm, zf_buf.at[col], load_sem.at[3]),
        pltpu.make_async_copy(mask_hbm, mask_buf, load_sem.at[4]),
        pltpu.make_async_copy(inner_hbm, inner, load_sem.at[5]),
        pltpu.make_async_copy(turn_hbm, turn, load_sem.at[6]),
        pltpu.make_async_copy(outer_hbm, outer, load_sem.at[7]),
    ]
    for load in loads:
        load.start()

    has_left, has_right = row > 0, row < R - 1
    barrier = pltpu.get_barrier_semaphore()

    def there(hop):
        return (row + hop < R) if hop > 0 else (row + hop >= 0)

    for hop in (-1, 1):
        @pl.when(there(hop))
        def _():
            pl.semaphore_signal(barrier, inc=1, device_id={"row": row + hop}, device_id_type=MESH)

    for step in range(1, C):
        pl.semaphore_signal(barrier, inc=1, device_id={"col": lax.rem(col + step, C)}, device_id_type=MESH)
    pl.semaphore_wait(barrier, C - 1 + jnp.where(has_left, 1, 0) + jnp.where(has_right, 1, 0))

    def tell(hop):
        far = abs(hop) + 1
        back = -1 if hop > 0 else 1
        if far <= reach:
            @pl.when(there(hop) & there(back))
            def _():
                pl.semaphore_signal(ready.at[int(hop < 0), far], inc=1,
                                    device_id={"row": row + back}, device_id_type=MESH)

    def learn(hop):
        @pl.when(there(hop))
        def _():
            pl.semaphore_wait(ready.at[int(hop < 0), abs(hop)], 1)

    tell(1)
    tell(-1)

    def spectrum(owner, w, send, to):
        return pltpu.make_async_remote_copy(
            n_buf.at[owner, w], n_buf.at[owner, w], send.at[owner, w], n_recv.at[owner, w],
            device_id={"row": to}, device_id_type=MESH)

    def flag(owner, send, to):
        return pltpu.make_async_remote_copy(
            nf_buf.at[owner], nf_buf.at[owner], send.at[owner], nf_recv.at[owner],
            device_id={"row": to}, device_id_type=MESH)

    def z_copy(owner, w, to):
        return pltpu.make_async_remote_copy(
            z_buf.at[owner, w], z_buf.at[owner, w], z_send.at[to, w], z_recv.at[owner, w],
            device_id={"col": to}, device_id_type=MESH)

    def zf_copy(owner, to):
        return pltpu.make_async_remote_copy(
            zf_buf.at[owner], zf_buf.at[owner], zf_send.at[to], zf_recv.at[owner],
            device_id={"col": to}, device_id_type=MESH)

    def own_copy(hop, w):
        side, far = int(hop < 0), abs(hop) - 1
        return pltpu.make_async_remote_copy(
            n_buf.at[row, w], n_buf.at[row, w], own_send.at[side, far, w], n_recv.at[row, w],
            device_id={"row": row + hop}, device_id_type=MESH)

    def own_flag(hop):
        side, far = int(hop < 0), abs(hop) - 1
        return pltpu.make_async_remote_copy(
            nf_buf.at[row], nf_buf.at[row], own_f_send.at[side, far], nf_recv.at[row],
            device_id={"row": row + hop}, device_id_type=MESH)

    pairs = C % 2 == 0
    first = (lax.rem(col, 2) == 0) if pairs else (col >= 0)

    def send_own(hop):
        @pl.when(there(hop))
        def _():
            own_flag(hop).start()
            for w in range(W):
                own_copy(hop, w).start()

    for hop in range(2, reach + 1):
        learn(-hop)
        tell(-hop)
    loads[2].wait()
    loads[0].wait()
    @pl.when(first)
    def _():
        for hop in range(reach, 0, -1):
            send_own(-hop)

    send_own(1)
    loads[3].wait()
    loads[1].wait()
    for step in range(1, C):
        zf_copy(col, lax.rem(col + step, C)).start()
    for w in range(W):
        for step in range(1, C):
            z_copy(col, w, lax.rem(col + step, C)).start()
    @pl.when(first)
    def _():
        for hop in range(1, reach + 1):
            @pl.when((row == hop) | ((row > hop) & (hop == reach)))
            def _():
                for w in range(W):
                    own_copy(-hop, w).wait_send()

        if pairs:
            pl.semaphore_signal(turn_sem, inc=1, device_id={"col": lax.rem(col + 1, C)}, device_id_type=MESH)

    @pl.when(jnp.logical_not(first))
    def _():
        send_own(-1)
        held = row == R - 1

        @pl.when(held)
        def _():
            pl.semaphore_wait(turn_sem, 1)

        for hop in range(reach, 1, -1):
            send_own(-hop)

        @pl.when(jnp.logical_not(held))
        def _():
            pl.semaphore_wait(turn_sem, 1)

    for hop in range(2, reach + 1):
        learn(hop)
        tell(hop)
        send_own(hop)
    for load in loads[4:]:
        load.wait()

    spot = lax.broadcasted_iota(jnp.int32, (bin_rows, LANES), 0) + lax.broadcasted_iota(
        jnp.int32, (bin_rows, LANES), 1)
    weight = jnp.where(spot == 0, 1.0, 2.0).astype(jnp.float32)

    def unit(owner):
        pairs = [(i, w) for i in range(C) for w in range(W)]
        n_real = [n_buf[owner, w, pl.ds(0, bin_rows, stride=2), :] * weight for w in range(W)]
        n_imag = [n_buf[owner, w, pl.ds(1, bin_rows, stride=2), :] * weight for w in range(W)]
        cross = []
        for i, w in pairs:
            z_real = z_buf[i, w, pl.ds(0, bin_rows, stride=2), :]
            z_imag = z_buf[i, w, pl.ds(1, bin_rows, stride=2), :]
            cross.append(jnp.concatenate(
                [z_real * n_real[w] + z_imag * n_imag[w], z_imag * n_real[w] - z_real * n_imag[w]], 0
            ).astype(jnp.bfloat16))
        short = jnp.dot(inner[...], jnp.concatenate(cross, 1), preferred_element_type=jnp.float32)
        turned = []
        for at in range(len(pairs)):
            real = short[:period, at * LANES:(at + 1) * LANES]
            imag = short[period:, at * LANES:(at + 1) * LANES]
            for part in range(LANES // period):
                cosine = turn[0, part * period:(part + 1) * period, :]
                sine = turn[1, part * period:(part + 1) * period, :]
                turned.append(jnp.concatenate(
                    [real * cosine - imag * sine, real * sine + imag * cosine], 1).astype(jnp.bfloat16))
        lags = lax.dot_general(outer[...], jnp.concatenate(turned, 0), (((1,), (1,)), ((), ())),
                               preferred_element_type=jnp.float32)
        lags = lags[:blocks] + lags[blocks:]
        n_flag = nf_buf[owner].astype(jnp.float32)
        mask = mask_buf[...].astype(jnp.float32)
        here = lax.broadcasted_iota(jnp.int32, mask.shape, 1) == owner
        kept = jnp.sum(jnp.where(here, mask, 0.0), axis=1, keepdims=True)
        for i in range(C):
            marks = zf_buf[i].astype(jnp.float32) * n_flag
            count = jnp.maximum(jnp.sum(marks, axis=1, keepdims=True), 1.0)
            gain = marks * kept[i:i + 1] / count
            total = jnp.zeros((blocks, LANES), jnp.float32)
            for w in range(W):
                at = i * W + w
                corr = lags[:, at * LANES:(at + 1) * LANES]
                power = jnp.sum(jnp.sum(corr * corr, axis=0, keepdims=True), axis=1, keepdims=True)
                spread = jnp.sqrt(power / LAGS + 1e-05)
                total = total + corr * (gain[:, w:w + 1] / spread)
            out_ref[pl.ds(i * blocks * R + owner, blocks, stride=R), :] = total

    def arrive(owner, w, forward, send, f_send, to):
        if w == 0:
            flag(owner, f_send, to).wait_recv()
        spectrum(owner, w, send, to).wait_recv()
        if forward is False:
            return

        @pl.when(forward)
        def _():
            if w == 0:
                flag(owner, f_send, to).start()
            spectrum(owner, w, send, to).start()

    for step in range(1, C):
        zf_copy(lax.rem(col + C - step, C), lax.rem(col + step, C)).wait_recv()
    for w in range(W):
        for step in range(1, C):
            z_copy(lax.rem(col + C - step, C), w, lax.rem(col + step, C)).wait_recv()
    unit(row)

    def take(p):
        left = p <= row
        owner = jnp.where(left, row - p, p)
        if reach == R - 1:
            for w in range(W):
                arrive(owner, w, False, right_send, rf_send, lax.rem(row + 1, R))
        else:
            @pl.when(left)
            def _():
                for w in range(W):
                    arrive(owner, w, has_right & (p >= reach), right_send, rf_send, lax.rem(row + 1, R))

            @pl.when(p > row)
            def _():
                for w in range(W):
                    arrive(owner, w, has_left & (p - row >= reach), left_send, lf_send,
                           lax.rem(row + R - 1, R))
        unit(owner)

    if R <= 4:
        for p in range(1, R):
            take(p)
    else:
        pl.loop(1, R)(take)

    hops = [sign * hop for hop in range(1, reach + 1) for sign in (1, -1)]
    for hop in hops:
        @pl.when(there(hop))
        def _():
            own_flag(hop).wait_send()
            if hop > 0:
                for w in range(W):
                    own_copy(hop, w).wait_send()
            else:
                waited = first & ((row == -hop) | ((row > -hop) & (-hop == reach)))

                @pl.when(jnp.logical_not(waited))
                def _():
                    for w in range(W):
                        own_copy(hop, w).wait_send()

    for step in range(1, C):
        zf_copy(col, lax.rem(col + step, C)).wait_send()
        for w in range(W):
            z_copy(col, w, lax.rem(col + step, C)).wait_send()

    if reach == R - 1:
        return

    @pl.loop(0, R)
    def _(owner):
        @pl.when(has_right & (owner <= row - reach))
        def _():
            flag(owner, rf_send, lax.rem(row + 1, R)).wait_send()
            for w in range(W):
                spectrum(owner, w, right_send, lax.rem(row + 1, R)).wait_send()

        @pl.when(has_left & (owner >= row + reach))
        def _():
            flag(owner, lf_send, lax.rem(row + R - 1, R)).wait_send()
            for w in range(W):
                spectrum(owner, w, left_send, lax.rem(row + R - 1, R)).wait_send()


def body(R, C, z_spectra, n_spectra, z_flags, n_flags, pair_mask):
    windows, bins = z_spectra.shape[1], z_spectra.shape[3]
    rows, blocks = bins // LANES, LAGS // LANES
    inner, turn, outer = tables(bins)

    def interleave(x):
        return x.reshape(1, windows, 2, rows, LANES).transpose(0, 1, 3, 2, 4).reshape(
            1, windows, 2 * rows, LANES)

    reach = min(REACH, R - 1)
    DMA = pltpu.SemaphoreType.DMA
    out = pl.pallas_call(
        functools.partial(kernel, R, C, reach),
        out_shape=pltpu.VMEM((C * blocks * R, LANES), jnp.float32),
        in_specs=[pl.BlockSpec(memory_space=pl.ANY)] * 8,
        out_specs=pl.BlockSpec(memory_space=pltpu.VMEM),
        scratch_shapes=[
            pltpu.VMEM((C, windows, 2 * rows, LANES), jnp.float32),
            pltpu.VMEM((R, windows, 2 * rows, LANES), jnp.float32),
            pltpu.VMEM((C, 1, windows), jnp.int32),
            pltpu.VMEM((R, 1, windows), jnp.int32),
            pltpu.VMEM(pair_mask.shape, jnp.int32),
            pltpu.VMEM(inner.shape, jnp.bfloat16),
            pltpu.VMEM(turn.shape, jnp.float32),
            pltpu.VMEM(outer.shape, jnp.bfloat16),
            DMA((8,)),
            DMA((C, windows)), DMA((C, windows)), DMA((C,)), DMA((C,)),
            DMA((R, windows)), DMA((R, windows)), DMA((R, windows)),
            DMA((R,)), DMA((R,)), DMA((R,)),
            DMA((2, reach, windows)), DMA((2, reach)), pltpu.SemaphoreType.REGULAR((2, reach + 1)),
            pltpu.SemaphoreType.REGULAR,
        ],
        compiler_params=pltpu.CompilerParams(collective_id=0, has_side_effects=True),
        name="correlate",
    )(interleave(z_spectra), interleave(n_spectra), z_flags, n_flags, pair_mask,
      jnp.asarray(inner), jnp.asarray(turn), jnp.asarray(outer))
    return out.reshape(C, blocks, R, LANES).transpose(0, 2, 1, 3).reshape(C, R, LAGS)


def solution(mesh):
    placed = (
        P(("grp", "row", "col"), None, None, None),
        P(("grp", "col", "row"), None, None, None),
        P(("grp", "row", "col"), None),
        P(("grp", "col", "row"), None),
        P(("grp", "row"), "col"),
    )
    return jax.shard_map(
        functools.partial(body, mesh.shape["row"], mesh.shape["col"]), mesh=mesh,
        in_specs=placed, out_specs=P(("grp", "row"), "col", None), check_vma=False,
    )
```
